32 devices in a mesh: row: 2 (over y), col: 8 (over z, x), layer: 2 (over core).
Axes of the slice: x: 2, y: 2, z: 4, core: 2. Of those that a mesh axis runs over, the one named last changes fastest.
Arguments:
- anomaly_x: bfloat16 [8, 4096, 4096], P(None, 'row', ('layer', 'col')), may hold values from -0.09375 to 0.09375
- anomaly_y: bfloat16 [8, 4096, 4096], P(None, 'col', ('layer', 'row')), may hold values from -6 to 6
Outputs:
- covariance: bfloat16 [8, 4096, 4096], P('layer', 'row', 'col')
The draws below stay inside these ranges and needn't reach their ends.
All inputs are finite; a program needn't handle non-finite values.
Results may differ from the reference program's by a relative error of at most 0.001.
Values may be sent and summed in bfloat16 or wider, within the bound.
No kernel may reach another device: no remote copies, remote signals or barrier semaphores. Data moves between devices by JAX's collectives and lax.ppermute only.
A program may use at most 192 MiB of HBM per device.

```python
import jax
import jax.numpy as jnp
from jax import lax

BATCH = 8
NSTATE = 4096
MEMBERS = 4096


def raised(values, own_key, source, target, shards_of, factor):
    owner, partner = [(jnp.arange(values.shape[axis_at]) // (values.shape[axis_at] // shards_of)).reshape([-1 if axis == axis_at else 1 for axis in range(values.ndim)]) for axis_at in (source, target)]
    chosen = jax.random.permutation(own_key, shards_of)[partner]
    strong = (owner == chosen) | (owner == (partner + shards_of // 2) % shards_of)
    return jnp.where(strong, factor * values, values)


def steps_of(rng, dims, cuts, least, top_value):
    level, own = 1.0, jax.random.fold_in(rng, 6)
    for position, shards_of in cuts:
        steps = jnp.exp(jax.random.uniform(jax.random.fold_in(own, position), (shards_of,), jnp.float32, least / len(cuts), top_value / len(cuts)))
        level = level * jnp.repeat(steps, dims[position] // shards_of).reshape([-1 if axis == position else 1 for axis in range(len(dims))])
    return level


def noise(rng, shape, deviation, reach, pieces=(), held_as=jnp.bfloat16):
    gain = steps_of(rng, shape, pieces, -0.22, 0.18) if pieces else 1.0
    drawn = jax.random.normal(rng, shape, jnp.float32) * deviation * gain
    return jnp.minimum(jnp.maximum(drawn, -reach), reach).astype(held_as)


def heavy_noise(stream_key, dims, deviation, reach, shards, heavy, kind=jnp.bfloat16):
    result = deviation * jax.random.normal(stream_key, dims, jnp.float32)
    if shards:
        result = result * steps_of(stream_key, dims, shards, -0.22, 0.18)
    return jnp.clip(raised(result, jax.random.fold_in(stream_key, 3), *heavy), -reach, reach).astype(kind)


def setup_inputs(seed: int = 0) -> dict:
    key_of = jax.random.split(jax.random.key(seed), 3)
    return {
        "anomaly_x": noise(key_of[0], (BATCH, NSTATE, MEMBERS), MEMBERS ** -0.5, 0.09375, ((1, 2), (2, 16))),
        "anomaly_y": heavy_noise(key_of[1], (BATCH, NSTATE, MEMBERS), 1.0, 6.0, ((1, 8), (2, 4)), (2, 0, 4, 2.0)),
    }


def one_product(pair):
    left, right = pair
    return jnp.dot(left, right.T, preferred_element_type=jnp.float32).astype(jnp.bfloat16)


def reference(anomaly_x, anomaly_y):
    return lax.map(one_product, (anomaly_x, anomaly_y))
```

```python
import jax
import jax.numpy as jnp
from jax import lax
from jax.sharding import Mesh, PartitionSpec as P

CHUNKS = 8


def gathered(anomaly_x, anomaly_y):
    panel_x = lax.all_gather(anomaly_x, "col", axis=2, tiled=True)
    partial_tile = jnp.einsum(
        "bik,bjk->bij",
        panel_x,
        lax.all_gather(anomaly_y, "row", axis=2, tiled=True),
        preferred_element_type=jnp.float32,
    )
    summed = lax.psum_scatter(partial_tile, "layer", scatter_dimension=0, tiled=True)
    return summed.astype(jnp.bfloat16)


def line(sizes, chunks, x, y):
    nrow, nz, nx, nlayer = (sizes[a] for a in ("row", "z", "x", "layer"))
    batch, rows, kx = x.shape
    _, cols, ky = y.shape
    part = rows // chunks
    z = lax.axis_index("z")
    inner = (z > 0) & (z < nz - 1)
    upper = z >= nz // 2
    inward = [(0, 1), (nz - 1, nz - 2)]
    outward = [(b, a) for a, b in inward]
    middle = [(nz // 2 - 1, nz // 2), (nz // 2, nz // 2 - 1)]
    blocks = ky // kx

    y = y.reshape(batch, cols, blocks, kx).transpose(0, 2, 1, 3).reshape(batch, blocks * cols, kx)

    def spread(a):
        return lax.all_to_all(a, ("layer", "row", "x"), 0, 0, tiled=True)

    def cut(a, q):
        return a[:, q * part : (q + 1) * part]

    first, o1, m1, second, o2, m2 = [], [], [], [], [], []
    for q in range(chunks):
        w = spread(jnp.where(inner, cut(x, q), cut(y, q)))
        first.append(w)
        o1.append(lax.ppermute(w, "z", inward))
        m1.append(lax.ppermute(w, "z", middle))
    for q in range(chunks):
        v = spread(jnp.where(inner, cut(y, q), cut(x, q)))
        second.append(v)
        o2.append(lax.ppermute(v, "z", inward))
        m2.append(lax.ppermute(o2[-1], "z", middle))

    def columns(pieces):
        a = jnp.concatenate(pieces, 1).reshape(nlayer, nrow, nx, blocks, cols, kx)
        return a.transpose(2, 4, 0, 1, 3, 5).reshape(nx * cols, nlayer * nrow * blocks * kx)

    right = jnp.concatenate([columns(second), columns(o1)], 0)
    out = []
    for q in range(chunks):
        held = [o2[q], first[q], m1[q], m2[q]]
        left = jnp.where(upper, jnp.stack(held[::-1]), jnp.stack(held))
        left = left.reshape(nz, nlayer, nrow, nx, part, kx).transpose(2, 4, 1, 0, 3, 5)
        left = left.reshape(nrow * part, nlayer * nz * nx * kx)
        c = lax.dot_general(left, right, (((1,), (1,)), ((), ())), preferred_element_type=jnp.float32)
        c = c.astype(jnp.bfloat16)
        own, other = c[:, : nx * cols], c[:, nx * cols :]
        tile = jnp.where(inner, own, lax.ppermute(other, "z", outward))
        tile = tile.reshape(nrow, part, nx, cols).transpose(0, 2, 1, 3).reshape(nrow * nx, part, cols)
        out.append(lax.all_to_all(tile, ("row", "x"), 0, 0, tiled=True))
    return jnp.concatenate(out, 1)


def line_sizes(mesh):
    coords = [getattr(d, "coords", None) for d in mesh.devices[0, :, 0]]
    if any(c is None for c in coords):
        return None
    nx = len({c[0] for c in coords})
    return {
        "row": mesh.shape["row"],
        "z": mesh.shape["col"] // nx,
        "x": nx,
        "layer": mesh.shape["layer"],
    }


def solution(mesh):
    sizes = line_sizes(mesh)

    def run(anomaly_x, anomaly_y):
        batch, nstate, members = anomaly_x.shape
        fits = sizes is not None and sizes["row"] * sizes["x"] * sizes["layer"] == batch and sizes["z"] == 4
        if not fits:
            placed = (P(None, "row", ("layer", "col")), P(None, "col", ("layer", "row")))
            return jax.shard_map(
                gathered, mesh=mesh, in_specs=placed, out_specs=P("layer", "row", "col"), check_vma=False
            )(anomaly_x, anomaly_y)
        names = ("row", "z", "x", "layer")
        split = Mesh(mesh.devices.reshape([sizes[a] for a in names]), names)
        placed = (P(None, "row", ("layer", "z", "x")), P(None, ("z", "x"), ("layer", "row")))
        return jax.shard_map(
            lambda x, y: line(sizes, CHUNKS, x, y),
            mesh=split,
            in_specs=placed,
            out_specs=P("layer", "row", ("z", "x")),
            check_vma=False,
        )(anomaly_x, anomaly_y)

    return run
```

```python
import jax
import jax.numpy as jnp
from jax import lax
from jax.experimental import pallas as pl
from jax.experimental.pallas import tpu as pltpu
from jax.sharding import Mesh, PartitionSpec as P


def gathered(anomaly_x, anomaly_y):
    panel_x = lax.all_gather(anomaly_x, "col", axis=2, tiled=True)
    partial_tile = jnp.einsum(
        "bik,bjk->bij",
        panel_x,
        lax.all_gather(anomaly_y, "row", axis=2, tiled=True),
        preferred_element_type=jnp.float32,
    )
    summed = lax.psum_scatter(partial_tile, "layer", scatter_dimension=0, tiled=True)
    return summed.astype(jnp.bfloat16)


def tile_kernel(upper_ref, *refs):
    xs, ys, out_ref = refs[:4], refs[4:8], refs[8]
    upper = upper_ref[0]
    nlayer, _, nx = xs[0].shape[:3]
    left, right = [], []
    for l in range(nlayer):
        for x_ref, (r, h) in zip(xs, ((0, 0), (0, 1), (1, 0), (1, 1))):
            for xx in range(nx):
                left.append(x_ref[l, 0, xx])
                right.append(ys[h * nx + xx][l, r ^ upper, 0])
    c = lax.dot_general(
        jnp.concatenate(left, 1),
        jnp.concatenate(right, 1),
        (((1,), (1,)), ((), ())),
        preferred_element_type=jnp.float32,
    )
    out_ref[0] = c.astype(out_ref.dtype)


def tiles(upper, outer, own, across, beyond, own_row, part, ys, dims):
    nrow, nx, nlayer = dims
    cols, kx = ys[0].shape[1:]
    shape5 = lambda a: a.reshape(nlayer, nrow, nx, *a.shape[1:])
    x_spec = lambda at: pl.BlockSpec((nlayer, 1, nx, part, kx), lambda j, i, u: (0, i, 0, at, 0))
    y_spec = pl.BlockSpec((nlayer, nrow, 1, cols, kx), lambda j, i, u: (0, 0, j, 0, 0))
    at = own_row // part
    depth = nlayer * 4 * nx * kx
    return pl.pallas_call(
        tile_kernel,
        grid_spec=pltpu.PrefetchScalarGridSpec(
            num_scalar_prefetch=1,
            grid=(nx, nrow),
            in_specs=[x_spec(0), x_spec(at), x_spec(at), x_spec(0)] + [y_spec] * 4,
            out_specs=pl.BlockSpec((1, part, cols), lambda j, i, u: (i * nx + j, 0, 0)),
        ),
        out_shape=jax.ShapeDtypeStruct((nrow * nx, part, cols), jnp.bfloat16),
        compiler_params=pltpu.CompilerParams(vmem_limit_bytes=48 << 20),
        cost_estimate=pl.CostEstimate(
            flops=2 * nrow * nx * part * cols * depth,
            bytes_accessed=2 * nx * depth * (nrow * part + cols),
            transcendentals=0,
        ),
    )(upper, *(shape5(a) for a in (outer, own, across, beyond)), *(shape5(a) for a in ys))


def pieces_of(blocks, cols):
    whole = [(c, 0, cols) for c in range(blocks - 1)]
    return whole + [(blocks - 1, 0, cols // 2), (blocks - 1, cols // 2, cols // 4), (blocks - 1, 3 * cols // 4, cols // 4)]


def line(sizes, x, y):
    nrow, nz, nx, nlayer = (sizes[a] for a in ("row", "z", "x", "layer"))
    _, rows, kx = x.shape
    _, cols, ky = y.shape
    z = lax.axis_index("z")
    inner = (z > 0) & (z < nz - 1)
    upper = z >= nz // 2
    inward = [(0, 1), (nz - 1, nz - 2)]
    outward = [(b, a) for a, b in inward]
    middle = [(nz // 2 - 1, nz // 2), (nz // 2, nz // 2 - 1)]
    blocks = ky // kx
    dims = (nrow, nx, nlayer)

    def permute(a, pairs):
        return lax.ppermute(a, "z", pairs)

    def spread(a):
        return lax.all_to_all(a, ("layer", "row", "x"), 0, 0, tiled=True)

    def x_block(c):
        return x[:, c * cols : (c + 1) * cols]

    def y_block(c):
        d = (c + blocks // 2) % blocks
        return jnp.where(upper, y[:, :, d * kx : (d + 1) * kx], y[:, :, c * kx : (c + 1) * kx])

    w, v, o1, m1 = [None] * blocks, [None] * blocks, [None] * blocks, [None] * blocks
    for c in range(blocks):
        w[c] = spread(jnp.where(inner, x_block(c), y_block(c)))
        o1[c] = permute(w[c], inward)
        m1[c] = permute(w[c], middle)
        v[c] = spread(jnp.where(inner, y_block(c), x_block(c)))
    flag = upper.astype(jnp.int32).reshape(1)
    out = jnp.zeros((nrow * nx, rows, cols), jnp.bfloat16)
    for c, first, part in pieces_of(blocks, cols):
        o2 = permute(v[c][:, first : first + part], inward)
        m2 = permute(o2, middle)
        far = tiles(flag, o2, w[c], m1[c], m2, first, part, o1, dims)
        near = tiles(flag, o2, w[c], m1[c], m2, first, part, v, dims)
        tile = jnp.where(inner, near, permute(far, outward))
        done = lax.all_to_all(tile, ("row", "x"), 0, 0, tiled=True)
        out = lax.dynamic_update_slice(out, done, (0, c * cols + first, 0))
    return out


def line_sizes(mesh):
    coords = [getattr(d, "coords", None) for d in mesh.devices[0, :, 0]]
    if any(c is None for c in coords):
        return None
    nx = len({c[0] for c in coords})
    return {
        "row": mesh.shape["row"],
        "z": mesh.shape["col"] // nx,
        "x": nx,
        "layer": mesh.shape["layer"],
    }


def fits(sizes, batch):
    return (
        sizes is not None
        and sizes["row"] * sizes["x"] * sizes["layer"] == batch
        and sizes["z"] == 2 * sizes["row"] == 2 * sizes["x"] == 4
    )


def solution(mesh):
    sizes = line_sizes(mesh)
    names = ("row", "z", "x", "layer")

    def plain(anomaly_x, anomaly_y):
        placed = (P(None, "row", ("layer", "col")), P(None, "col", ("layer", "row")))
        return jax.shard_map(
            gathered, mesh=mesh, in_specs=placed, out_specs=P("layer", "row", "col"), check_vma=False
        )(anomaly_x, anomaly_y)

    def body(x, y):
        return line(sizes, x, y)

    def lined(anomaly_x, anomaly_y):
        split = Mesh(mesh.devices.reshape([sizes[a] for a in names]), names)
        placed = (P(None, "row", ("layer", "z", "x")), P(None, ("z", "x"), ("layer", "row")))
        step = jax.shard_map(
            body, mesh=split, in_specs=placed, out_specs=P("layer", "row", ("z", "x")), check_vma=False
        )
        return step(anomaly_x, anomaly_y)

    def run(anomaly_x, anomaly_y):
        return (lined if fits(sizes, anomaly_x.shape[0]) else plain)(anomaly_x, anomaly_y)

    return run
```
